32 devices in a mesh: dp: 4 (over y, z), tp: 8 (over x, core).
Axes of the slice: x: 4, y: 2, z: 2, core: 2. Of those that a mesh axis runs over, the one named last changes fastest.
The devices are a block of a 4x4x8 slice.
Arguments:
- X: bfloat16 [1024, 2560], P(('dp', 'tp')), parts along dimension 0
- dY: bfloat16 [1024, 2560], P(('dp', 'tp')), parts along dimension 0
- W1: bfloat16 [2560, 10240], P(None, 'tp')
- W2: bfloat16 [10240, 2560], P('tp')
Outputs:
- output 1: bfloat16 [1024, 2560], P(('dp', 'tp')), parts along dimension 0
- output 2: float32 [10240, 10240], P('dp', 'tp'), parts along dimension 0
- output 3: float32 [40960, 2560], P(('dp', 'tp')), parts along dimension 0
There are 4 independent parts. The reference program is written for one: setup_inputs(seed, part) draws one part's arguments, and reference() takes and returns one part's arrays. A program takes and returns all parts, laid end to end along the dimension named above; an argument that names none is the same for every part.
All inputs are finite; a program needn't handle non-finite values.
Results may differ from the reference program's by a relative error of at most 0.00938058.
Values are sent between devices in bfloat16 or wider.
A program may use at most 768 MiB of HBM per device.

```python
import math
import jax
import jax.numpy as jnp
from jax import lax

TP = 8
TOKENS_DEV = 32
H = 2560
FF_DEV = 1280

T = TOKENS_DEV * TP
F = FF_DEV * TP
C0 = math.sqrt(2.0 / math.pi)
C1 = 0.044715


def _gelu(u):
    t = jnp.tanh(C0 * (u + C1 * u * u * u))
    return 0.5 * u * (1.0 + t), 0.5 * (1.0 + t) + 0.5 * u * (1.0 - t * t) * C0 * (1.0 + 3.0 * C1 * u * u)


def setup_inputs(seed: int = 0, part: int = 0) -> dict:
    key = jax.random.PRNGKey(seed)
    ks = jax.random.split(key, 3)
    kx, kdy = jax.random.split(jax.random.fold_in(ks[0], part))
    x = jax.random.normal(kx, (T, H), jnp.float32).astype(jnp.bfloat16)
    dy = jax.random.normal(kdy, (T, H), jnp.float32).astype(jnp.bfloat16)
    w1 = (jax.random.normal(ks[1], (H, F), jnp.float32) * H ** -0.5).astype(jnp.bfloat16)
    w2 = (jax.random.normal(ks[2], (F, H), jnp.float32) * F ** -0.5).astype(jnp.bfloat16)
    return {'X': x, 'dY': dy, 'W1': w1, 'W2': w2}


def reference(X, dY, W1, W2):
    w1c = W1.reshape(H, TP, FF_DEV).transpose(1, 0, 2)
    w2c = W2.reshape(TP, FF_DEV, H)

    def step(acc, w):
        a, b = w
        u = jnp.dot(X, a, preferred_element_type=jnp.float32).astype(jnp.bfloat16)
        g0, g1 = _gelu(u.astype(jnp.float32))
        z = g0.astype(jnp.bfloat16)
        dw2 = jnp.dot(z.T, dY, preferred_element_type=jnp.float32)
        g = jnp.dot(dY, b.T, preferred_element_type=jnp.float32)
        dz = (g * g1).astype(jnp.bfloat16)
        acc = acc + jnp.dot(dz, a.T, preferred_element_type=jnp.float32)
        dw1 = jnp.dot(X.T, dz, preferred_element_type=jnp.float32)
        return acc, (dw1, dw2)

    acc, (dw1, dw2) = lax.scan(step, jnp.zeros((T, H), jnp.float32), (w1c, w2c))
    dX = acc.astype(jnp.bfloat16)
    dW1 = dw1.transpose(1, 0, 2).reshape(H, F)
    dW2 = dw2.reshape(F, H)
    return (dX, dW1, dW2)
```

```python
import functools
import math
import jax
import jax.numpy as jnp
from jax import lax
from jax.experimental import pallas as pl
from jax.experimental.pallas import tpu as pltpu
from jax.sharding import PartitionSpec as P

C0 = math.sqrt(2.0 / math.pi)
C1 = 0.044715
MESH = pl.DeviceIdType.MESH
F32, BF16 = jnp.float32, jnp.bfloat16


def _gelu(u):
    t = jnp.tanh(C0 * (u + C1 * u * u * u))
    return 0.5 * u * (1.0 + t), 0.5 * (1.0 + t) + 0.5 * u * (1.0 - t * t) * C0 * (1.0 + 3.0 * C1 * u * u)


def _nt(a, b):
    return lax.dot_general(a, b, (((1,), (1,)), ((), ())), preferred_element_type=F32)


def _tn(a, b):
    return lax.dot_general(a, b, (((0,), (0,)), ((), ())), preferred_element_type=F32)


def _chunks(width, sizes):
    out, at = [], 0
    for s in sizes:
        out.append(slice(at, at + s))
        at += s
    assert at == width
    return out


def _forward_kernel(n, rows, chunks, pchunks,
                    x_ref, dy_ref, w1_ref, w2_ref,
                    xg, dyg, z_ref, dz_ref, own_ref, plus_ref, minus_ref, oppa_ref, oppb_ref,
                    w1_s, w2_s, u_s, g_s, keep_s, psend, precv,
                    lsem, ssem, rsem, pss, prs):
    half = n // 2
    me = lax.axis_index('tp')
    chip, core = me // 2, me % 2
    right = ((chip + 1) % half) * 2 + core
    left = ((chip + half - 1) % half) * 2 + core
    mate = chip * 2 + (1 - core)
    h = rows // 2

    def blk(s, d, lo=0, size=rows):
        return pl.ds((s * half + d) * rows + lo, size)

    loc = [pltpu.make_async_copy(x_ref, xg.at[blk(0, 0)], lsem.at[0]),
           pltpu.make_async_copy(dy_ref, dyg.at[blk(0, 0)], lsem.at[1]),
           pltpu.make_async_copy(w1_ref, w1_s, lsem.at[2]),
           pltpu.make_async_copy(w2_ref, w2_s, lsem.at[3])]
    for c in loc:
        c.start()

    barrier = pltpu.get_barrier_semaphore()
    for peer in (mate, left, right):
        pl.semaphore_signal(barrier, inc=1, device_id={'tp': peer}, device_id_type=MESH)
    pl.semaphore_wait(barrier, 3)

    def copies(buf, a, j):
        cols = chunks[j]

        def cp(kind, src, dst, dev):
            return pltpu.make_async_remote_copy(
                src_ref=buf.at[src, cols], dst_ref=buf.at[dst, cols],
                send_sem=ssem.at[a, j, kind], recv_sem=rsem.at[a, j, kind],
                device_id={'tp': dev}, device_id_type=MESH)

        return dict(
            np=cp(0, blk(0, 0), blk(0, 3), right),
            nm=cp(1, blk(0, 0), blk(0, 1), left),
            p0=cp(2, blk(0, 0), blk(1, 0), mate),
            fp=cp(3, blk(0, 3, 0, h), blk(0, 2, 0, h), right),
            fm=cp(4, blk(0, 1, h, h), blk(0, 2, h, h), left),
            p3=cp(5, blk(0, 3), blk(1, 3), mate),
            p1=cp(6, blk(0, 1), blk(1, 1), mate),
            p2a=cp(7, blk(0, 2, 0, h), blk(1, 2, 0, h), mate),
            p2b=cp(8, blk(0, 2, h, h), blk(1, 2, h, h), mate))

    nj = len(chunks)
    cx = [copies(xg, 0, j) for j in range(nj)]
    cy = [copies(dyg, 1, j) for j in range(nj)]

    def first(c):
        c['np'].start()
        c['nm'].start()
        c['p0'].start()

    def second(c):
        c['np'].wait_recv()
        c['fp'].start()
        c['p3'].start()
        c['nm'].wait_recv()
        c['fm'].start()
        c['p1'].start()

    def third(c):
        c['fp'].wait_recv()
        c['p2a'].start()
        c['fm'].wait_recv()
        c['p2b'].start()

    def last(c):
        for k in ('p0', 'p3', 'p1', 'p2a', 'p2b'):
            c[k].wait_recv()

    loc[0].wait()
    for c in cx:
        first(c)
    loc[1].wait()
    for c in cy:
        first(c)
    for c in cx:
        second(c)
    for c in cy:
        second(c)
    loc[2].wait()
    for j, c in enumerate(cx):
        third(c)
        last(c)
        part = jnp.dot(xg[:, chunks[j]], w1_s[chunks[j], :], preferred_element_type=F32)
        if j == 0:
            u_s[...] = part
        else:
            u_s[...] += part
    for c in cy[:-1]:
        third(c)

    @pl.loop(0, u_s.shape[0] // 16)
    def _(i):
        r = pl.ds(pl.multiple_of(i * 16, 16), 16)
        u = u_s[r, :].astype(BF16).astype(F32)
        g0, g1 = _gelu(u)
        z_ref[r, :] = g0.astype(BF16)
        u_s[r, :] = g1

    loc[3].wait()
    for j, c in enumerate(cy):
        if j == nj - 1:
            third(c)
        last(c)
        part = _nt(dyg[:, chunks[j]], w2_s[:, chunks[j]])
        if j == 0:
            g_s[...] = part
        else:
            g_s[...] += part

    @pl.loop(0, u_s.shape[0] // 16)
    def _(i):
        r = pl.ds(pl.multiple_of(i * 16, 16), 16)
        dz_ref[r, :] = (g_s[r, :] * u_s[r, :]).astype(BF16)

    m = half * rows
    pc = []
    for j, cols in enumerate(pchunks):
        part = _nt(dz_ref[...], w1_s[cols, :])
        psend[:, cols] = part[m:].astype(BF16)
        c = pltpu.make_async_remote_copy(
            src_ref=psend.at[:, cols], dst_ref=precv.at[:, cols], send_sem=pss.at[j], recv_sem=prs.at[j],
            device_id={'tp': mate}, device_id_type=MESH)
        c.start()
        pc.append(c)
        keep_s[:, cols] = part[:m]
    for j, cols in enumerate(pchunks):
        pc[j].wait_recv()

        def red(d, lo=0, size=rows):
            r = slice(d * rows + lo, d * rows + lo + size)
            return keep_s[r, cols] + precv[r, cols].astype(F32)

        oppa_ref[:, cols] = red(2, 0, h).astype(BF16)
        oppb_ref[:, cols] = red(2, h, h).astype(BF16)
        plus_ref[:, cols] = red(1).astype(BF16)
        minus_ref[:, cols] = red(3).astype(BF16)
        own_ref[:, cols] = red(0)
    for c in cx + cy:
        for k in c.values():
            k.wait_send()
    for c in pc:
        c.wait_send()


def _forward(x, dy, w1, w2, n):
    rows, hid = x.shape
    ff = w1.shape[1]
    t = rows * n
    chunks = _chunks(hid, (768, 768, 512, 512))
    pchunks = _chunks(hid, (512,) * 5)
    vm = pl.BlockSpec(memory_space=pltpu.VMEM)
    hbm = pl.BlockSpec(memory_space=pltpu.MemorySpace.HBM)
    sd = jax.ShapeDtypeStruct
    dma = pltpu.SemaphoreType.DMA

    return pl.pallas_call(
        functools.partial(_forward_kernel, n, rows, chunks, pchunks),
        out_shape=(sd((t, hid), BF16), sd((t, hid), BF16), sd((t, ff), BF16), sd((t, ff), BF16),
                   sd((rows, hid), F32), sd((rows, hid), BF16), sd((rows, hid), BF16),
                   sd((rows // 2, hid), BF16), sd((rows // 2, hid), BF16)),
        in_specs=[hbm] * 4,
        out_specs=(vm,) * 9,
        scratch_shapes=[
            pltpu.VMEM((hid, ff), BF16), pltpu.VMEM((ff, hid), BF16),
            pltpu.VMEM((t, ff), F32), pltpu.VMEM((t, ff), F32),
            pltpu.VMEM((t // 2, hid), F32), pltpu.VMEM((t // 2, hid), BF16), pltpu.VMEM((t // 2, hid), BF16),
            dma((4,)), dma((2, len(chunks), 9)), dma((2, len(chunks), 9)),
            dma((len(pchunks),)), dma((len(pchunks),))],
        compiler_params=pltpu.CompilerParams(
            collective_id=0, has_side_effects=True, vmem_limit_bytes=36 << 20),
        name='gather_dz',
    )(*[pltpu.with_memory_space_constraint(v, pltpu.MemorySpace.HBM) for v in (x, dy, w1, w2)])


def _wgrad(a, b, bm, name):
    t, m = a.shape
    w = b.shape[1]

    def kernel(a_ref, b_ref, o_ref, buf, sem):
        copies = []
        for i in range(m // bm):
            r = slice(i * bm, (i + 1) * bm)
            buf[r, :] = _tn(a_ref[:, r], b_ref[...])
            copies.append(pltpu.make_async_copy(buf.at[r], o_ref.at[r], sem.at[i]))
            copies[-1].start()
        for c in copies:
            c.wait()

    vm = pl.BlockSpec(memory_space=pltpu.VMEM)
    return pl.pallas_call(
        kernel, out_shape=jax.ShapeDtypeStruct((m, w), F32), in_specs=[vm] * 2,
        out_specs=pl.BlockSpec(memory_space=pltpu.MemorySpace.HBM), name=name,
        scratch_shapes=[pltpu.VMEM((m, w), F32), pltpu.SemaphoreType.DMA((m // bm,))],
        compiler_params=pltpu.CompilerParams(vmem_limit_bytes=24 << 20),
        cost_estimate=pl.CostEstimate(flops=8 * t * m * w, bytes_accessed=4 * m * w, transcendentals=0))(a, b)


def solution(mesh):
    n = mesh.shape['tp']
    half = n // 2

    def body(x, dy, w1, w2):
        h = x.shape[0] // 2
        ahead = [(2 * k + c, 2 * ((k + 1) % half) + c) for k in range(half) for c in range(2)]
        back = [(b, a) for a, b in ahead]
        xg, dyg, z, dz, own, plus, minus, oppa, oppb = _forward(x, dy, w1, w2, n)
        ra = lax.ppermute(oppa, 'tp', ahead)
        rb = lax.ppermute(oppb, 'tp', back)
        dw2 = _wgrad(z, dyg, 256, 'dw2')
        plus = jnp.concatenate([(plus[:h].astype(F32) + ra.astype(F32)).astype(BF16), plus[h:]])
        minus = jnp.concatenate([minus[:h], (minus[h:].astype(F32) + rb.astype(F32)).astype(BF16)])
        qa = lax.ppermute(plus, 'tp', ahead)
        qb = lax.ppermute(minus, 'tp', back)
        dw1 = _wgrad(xg, dz, 256, 'dw1')
        dx = (own + qa.astype(F32) + qb.astype(F32)).astype(BF16)
        return dx, dw1, dw2

    return jax.shard_map(
        body, mesh=mesh,
        in_specs=(P(('dp', 'tp'), None), P(('dp', 'tp'), None), P(None, 'tp'), P('tp', None)),
        out_specs=(P(('dp', 'tp'), None), P('dp', 'tp'), P(('dp', 'tp'), None)),
        check_vma=False)
```

```python
import functools
import math
import jax
import jax.numpy as jnp
from jax import lax
from jax.experimental import pallas as pl
from jax.experimental.pallas import tpu as pltpu
from jax.sharding import PartitionSpec as P

C0 = math.sqrt(2.0 / math.pi)
C1 = 0.044715
MESH = pl.DeviceIdType.MESH
F32, BF16 = jnp.float32, jnp.bfloat16
XCH = (1280, 1280)
YCH = (1280, 1280)
YF = ((1280,), (768, 512))
PCH = (768, 768, 768, 256)
ORDER = ((0, 0), (0, 1), (0, 3), (1, 0), (1, 1), (1, 3), (0, 2), (1, 2))


def _gelu(u):
    t = jnp.tanh(C0 * (u + C1 * u * u * u))
    return 0.5 * u * (1.0 + t), 0.5 * (1.0 + t) + 0.5 * u * (1.0 - t * t) * C0 * (1.0 + 3.0 * C1 * u * u)


def _nt(a, b):
    return lax.dot_general(a, b, (((1,), (1,)), ((), ())), preferred_element_type=F32)


def _tn(a, b):
    return lax.dot_general(a, b, (((0,), (0,)), ((), ())), preferred_element_type=F32)


def _cols(sizes, at=0):
    out = []
    for s in sizes:
        out.append(slice(at, at + s))
        at += s
    return out


def _forward_kernel(n, rows,
                    x_ref, dy_ref, w1_ref, w2_ref,
                    xg, dyg, z_ref, dz_ref, own_ref, plus_ref, minus_ref, opp_ref,
                    w1_s, w2_s, u_s, g_s, keep_s, psend, precv,
                    lsem, ssem, rsem, pss, prs):
    half = n // 2
    me = lax.axis_index('tp')
    chip, core = me // 2, me % 2
    right = ((chip + 1) % half) * 2 + core
    left = ((chip + half - 1) % half) * 2 + core
    mate = chip * 2 + (1 - core)
    h = rows // 2
    near = (n - 2) * rows

    def blk(s, d, lo=0, size=rows):
        at = ORDER.index((s, d)) * rows + lo
        return slice(at, at + size)

    loc = [pltpu.make_async_copy(x_ref, xg.at[blk(0, 0)], lsem.at[0]),
           pltpu.make_async_copy(dy_ref, dyg.at[blk(0, 0)], lsem.at[1]),
           pltpu.make_async_copy(w1_ref, w1_s, lsem.at[2]),
           pltpu.make_async_copy(w2_ref, w2_s, lsem.at[3])]
    loc[0].start()
    loc[1].start()

    barrier = pltpu.get_barrier_semaphore()
    for peer in (mate, left, right):
        pl.semaphore_signal(barrier, inc=1, device_id={'tp': peer}, device_id_type=MESH)
    pl.semaphore_wait(barrier, 3)

    used = [0]
    started = []

    def remote(buf, src, dst, cols, dev):
        i = used[0]
        used[0] += 1
        c = pltpu.make_async_remote_copy(
            src_ref=buf.at[src, cols], dst_ref=buf.at[dst, cols], send_sem=ssem.at[i], recv_sem=rsem.at[i],
            device_id={'tp': dev}, device_id_type=MESH)
        started.append(c)
        return c

    def first(buf, sizes):
        out = []
        for cols in _cols(sizes):
            a = remote(buf, blk(0, 0), blk(0, 3), cols, right)
            b = remote(buf, blk(0, 0), blk(0, 1), cols, left)
            a.start()
            b.start()
            out.append((a, b))
        own = remote(buf, blk(0, 0), blk(1, 0), slice(None), mate)
        own.start()
        return out, own

    def second(buf, pair, cols, parts):
        fa, fb = [], []
        pair[0].wait_recv()
        for q in parts:
            fa.append(remote(buf, blk(0, 3, 0, h), blk(0, 2, 0, h), q, right))
            fa[-1].start()
        ra = remote(buf, blk(0, 3), blk(1, 3), cols, mate)
        ra.start()
        pair[1].wait_recv()
        for q in parts:
            fb.append(remote(buf, blk(0, 1, h, h), blk(0, 2, h, h), q, left))
            fb[-1].start()
        rb = remote(buf, blk(0, 1), blk(1, 1), cols, mate)
        rb.start()
        return list(zip(fa, fb)), (ra, rb)

    def third(buf, pair, cols):
        pair[0].wait_recv()
        pair[1].wait_recv()
        c = remote(buf, blk(0, 2), blk(1, 2), cols, mate)
        c.start()
        return c

    def wait_all(*cs):
        for c in cs:
            c.wait_recv()

    xc, yc = _cols(XCH), _cols(YCH)
    yf = [_cols(p, c.start) for p, c in zip(YF, yc)]
    loc[0].wait()
    nx, px = first(xg, XCH)
    loc[1].wait()
    ny, py = first(dyg, YCH)
    loc[2].start()
    loc[3].start()
    fx, rx = zip(*[second(xg, p, c, (c,)) for p, c in zip(nx, xc)])
    loc[2].wait()
    wait_all(px, *rx[0], *rx[1])
    u_s[:near, :] = jnp.dot(xg[:near, :], w1_s[...], preferred_element_type=F32)

    def act(lo, hi):
        @pl.loop(lo // 16, hi // 16)
        def _(i):
            r = pl.ds(pl.multiple_of(i * 16, 16), 16)
            u = u_s[r, :].astype(BF16).astype(F32)
            g0, g1 = _gelu(u)
            z_ref[r, :] = g0.astype(BF16)
            u_s[r, :] = g1

    fy, ry = [], []
    f, r = second(dyg, ny[0], yc[0], yf[0])
    fy += f
    ry += r
    act(0, near)
    f, r = second(dyg, ny[1], yc[1], yf[1])
    fy += f
    ry += r
    loc[3].wait()

    ox = []
    for j, c in enumerate(xc):
        ox.append(third(xg, fx[j][0], c))
    yq = [q for part in yf for q in part]
    oy = []
    for j, c in enumerate(xc):
        ox[j].wait_recv()
        part = jnp.dot(xg[near:, c], w1_s[c, :], preferred_element_type=F32)
        if j == 0:
            u_s[near:, :] = part
        else:
            u_s[near:, :] += part
        oy.append(third(dyg, fy[j], yq[j]))
    act(near, n * rows)
    wait_all(py, *ry)
    for j, q in enumerate(yq):
        if j == 1:
            for i in range(len(oy), len(yq)):
                oy.append(third(dyg, fy[i], yq[i]))
        oy[j].wait_recv()
        part = _nt(dyg[:, q], w2_s[:, q])
        if j == 0:
            g_s[...] = part
        else:
            g_s[...] += part

    @pl.loop(0, n * rows // 16)
    def _(i):
        r = pl.ds(pl.multiple_of(i * 16, 16), 16)
        dz_ref[r, :] = (g_s[r, :] * u_s[r, :]).astype(BF16)

    pcols = _cols(PCH)
    pc = []
    m = 3 * rows
    for j, cols in enumerate(pcols):
        part = _nt(dz_ref[...], w1_s[cols, :])
        psend[:m, cols] = part[m:2 * m].astype(BF16)
        psend[m:, cols] = part[2 * m + rows:].astype(BF16)
        c = pltpu.make_async_remote_copy(
            src_ref=psend.at[:, cols], dst_ref=precv.at[:, cols], send_sem=pss.at[j], recv_sem=prs.at[j],
            device_id={'tp': mate}, device_id_type=MESH)
        c.start()
        pc.append(c)
        keep_s[:m, cols] = part[:m]
        keep_s[m:, cols] = part[2 * m:2 * m + rows]
    for c in started:
        c.wait_send()
    for j, cols in enumerate(pcols):
        pc[j].wait_recv()
        tot = [keep_s[d * rows:(d + 1) * rows, cols] + precv[d * rows:(d + 1) * rows, cols].astype(F32)
               for d in range(half)]
        own_ref[:, cols] = tot[0]
        plus_ref[:, cols] = tot[1].astype(BF16)
        minus_ref[:, cols] = tot[2].astype(BF16)
        opp_ref[:, cols] = tot[3].astype(BF16)
    for c in pc:
        c.wait_send()


def _hbm(*arrays):
    return [pltpu.with_memory_space_constraint(v, pltpu.MemorySpace.HBM) for v in arrays]


def _forward(x, dy, w1, w2, n):
    rows, hid = x.shape
    ff = w1.shape[1]
    t = rows * n
    vm = pl.BlockSpec(memory_space=pltpu.VMEM)
    hbm = pl.BlockSpec(memory_space=pltpu.MemorySpace.HBM)
    sd = jax.ShapeDtypeStruct
    dma = pltpu.SemaphoreType.DMA
    ncopies = 64
    return pl.pallas_call(
        functools.partial(_forward_kernel, n, rows),
        out_shape=(sd((t, hid), BF16), sd((t, hid), BF16), sd((t, ff), BF16), sd((t, ff), BF16),
                   sd((rows, hid), F32), sd((rows, hid), BF16), sd((rows, hid), BF16), sd((rows, hid), BF16)),
        in_specs=[hbm] * 4,
        out_specs=(vm,) * 8,
        scratch_shapes=[
            pltpu.VMEM((hid, ff), BF16), pltpu.VMEM((ff, hid), BF16),
            pltpu.VMEM((t, ff), F32), pltpu.VMEM((t, ff), F32),
            pltpu.VMEM((t // 2, hid), F32), pltpu.VMEM((t // 2, hid), BF16), pltpu.VMEM((t // 2, hid), BF16),
            dma((4,)), dma((ncopies,)), dma((ncopies,)), dma((len(PCH),)), dma((len(PCH),))],
        compiler_params=pltpu.CompilerParams(
            collective_id=0, has_side_effects=True, vmem_limit_bytes=36 << 20),
        name='gather_dz',
    )(*_hbm(x, dy, w1, w2))


def _wgrads(pairs, bm):
    def kernel(*refs):
        k = len(pairs)
        ins, outs, bufs, sem = refs[:2 * k], refs[2 * k:3 * k], refs[3 * k:4 * k], refs[4 * k]
        copies = []
        for p in range(k):
            a_ref, b_ref, o_ref, buf = ins[2 * p], ins[2 * p + 1], outs[p], bufs[p]
            for i in range(o_ref.shape[0] // bm):
                r = slice(i * bm, (i + 1) * bm)
                buf[r, :] = _tn(a_ref[:, r], b_ref[...])
                copies.append(pltpu.make_async_copy(buf.at[r], o_ref.at[r], sem.at[len(copies)]))
                copies[-1].start()
        for c in copies:
            c.wait()

    vm = pl.BlockSpec(memory_space=pltpu.VMEM)
    shapes = [(a.shape[1], b.shape[1]) for a, b in pairs]
    nsem = sum(s[0] // bm for s in shapes)
    t = pairs[0][0].shape[0]
    size = sum(s[0] * s[1] for s in shapes)
    return pl.pallas_call(
        kernel, out_shape=[jax.ShapeDtypeStruct(s, F32) for s in shapes], in_specs=[vm] * (2 * len(pairs)),
        out_specs=[pl.BlockSpec(memory_space=pltpu.MemorySpace.HBM)] * len(pairs), name='wgrads',
        scratch_shapes=[pltpu.VMEM(s, F32) for s in shapes] + [pltpu.SemaphoreType.DMA((nsem,))],
        compiler_params=pltpu.CompilerParams(vmem_limit_bytes=36 << 20),
        cost_estimate=pl.CostEstimate(flops=8 * t * size, bytes_accessed=4 * size, transcendentals=0),
    )(*[v for p in pairs for v in p])


def solution(mesh):
    n = mesh.shape['tp']
    half = n // 2

    def hop(v, d):
        return lax.ppermute(v, 'tp', [(2 * k + c, 2 * ((k + d) % half) + c) for k in range(half) for c in range(2)])

    def body(x, dy, w1, w2):
        xg, dyg, z, dz, own, plus, minus, opp = _forward(x, dy, w1, w2, n)
        parts = [hop(opp, 2), hop(plus, 1), hop(minus, half - 1)]
        dw2, dw1 = _wgrads([(z, dyg), (xg, dz)], 256)
        dx = own
        for p in parts:
            dx = dx + p.astype(F32)
        return dx.astype(BF16), dw1, dw2

    return jax.shard_map(
        body, mesh=mesh,
        in_specs=(P(('dp', 'tp'), None), P(('dp', 'tp'), None), P(None, 'tp'), P('tp', None)),
        out_specs=(P(('dp', 'tp'), None), P('dp', 'tp'), P(('dp', 'tp'), None)),
        check_vma=False)
```

```python
import functools
import math
import jax
import jax.numpy as jnp
from jax import lax
from jax.experimental import pallas as pl
from jax.experimental.pallas import tpu as pltpu
from jax.sharding import PartitionSpec as P

C0 = math.sqrt(2.0 / math.pi)
C1 = 0.044715
MESH = pl.DeviceIdType.MESH
F32, BF16 = jnp.float32, jnp.bfloat16
XCH = (1280, 1280)
YCH = (1024, 1024, 512)
PCH = (1280, 1280)
ORDER = ((0, 0), (0, 1), (0, 3), (1, 0), (1, 1), (1, 3), (0, 2), (1, 2))


def _gelu(u):
    q = (3.0 * C0 * C1 * u) * u
    t = jnp.tanh(u * (C0 + q * (1.0 / 3.0)))
    p = 0.5 + 0.5 * t
    z = u * p
    return z, p + (z * (1.0 - t)) * (C0 + q)


def _nt(a, b):
    return lax.dot_general(a, b, (((1,), (1,)), ((), ())), preferred_element_type=F32)


def _tn(a, b):
    return lax.dot_general(a, b, (((0,), (0,)), ((), ())), preferred_element_type=F32)


def _cols(sizes, at=0):
    out = []
    for s in sizes:
        out.append(slice(at, at + s))
        at += s
    return out


def _forward_kernel(n, rows,
                    x_ref, dy_ref, w1_ref, w2_ref,
                    xg, dyg, z_ref, dz_ref, own_ref, plus_ref, minus_ref, opp_ref,
                    w1_s, w2_s, u_s, g_s, keep_s, psend, precv,
                    lsem, ssem, rsem, pss, prs):
    half = n // 2
    me = lax.axis_index('tp')
    chip, core = me // 2, me % 2
    right = ((chip + 1) % half) * 2 + core
    left = ((chip + half - 1) % half) * 2 + core
    mate = chip * 2 + (1 - core)
    h = rows // 2
    most = (n - 2) * rows

    def blk(s, d, lo=0, size=rows):
        at = ORDER.index((s, d)) * rows + lo
        return slice(at, at + size)

    loc = [pltpu.make_async_copy(x_ref, xg.at[blk(0, 0)], lsem.at[0]),
           pltpu.make_async_copy(dy_ref, dyg.at[blk(0, 0)], lsem.at[1]),
           pltpu.make_async_copy(w1_ref, w1_s, lsem.at[2]),
           pltpu.make_async_copy(w2_ref, w2_s, lsem.at[3])]
    loc[0].start()
    loc[1].start()

    barrier = pltpu.get_barrier_semaphore()
    for peer in (mate, left, right):
        pl.semaphore_signal(barrier, inc=1, device_id={'tp': peer}, device_id_type=MESH)
    pl.semaphore_wait(barrier, 3)

    used = [0]
    started = []

    def remote(buf, src, dst, cols, dev):
        i = used[0]
        used[0] += 1
        c = pltpu.make_async_remote_copy(
            src_ref=buf.at[src, cols], dst_ref=buf.at[dst, cols], send_sem=ssem.at[i], recv_sem=rsem.at[i],
            device_id={'tp': dev}, device_id_type=MESH)
        started.append(c)
        return c

    def first(buf, cols):
        a = remote(buf, blk(0, 0), blk(0, 3), cols, right)
        b = remote(buf, blk(0, 0), blk(0, 1), cols, left)
        a.start()
        b.start()
        return a, b

    def relay(buf, src, dst, cols):
        c = remote(buf, blk(*src), blk(*dst), cols, mate)
        c.start()
        return c

    def second(buf, pair, parts, both=()):
        out = []
        for k, (c, s, d, lo, dev, dev2) in enumerate((
                (pair[0], (0, 3), (0, 2), 0, right, right + 1 - 2 * core),
                (pair[1], (0, 1), (0, 2), h, left, left + 1 - 2 * core))):
            c.wait_recv()
            for q in parts:
                f = [remote(buf, blk(*s, lo, h), blk(*d, lo, h), q, dev)]
                if q in both:
                    f.append(remote(buf, blk(*s, lo, h), blk(1, 2, lo, h), q, dev2))
                for v in f:
                    v.start()
                out.append((q, f))
        return out

    def near(buf, cols):
        at = blk(0, 1).start, blk(1, 1).start
        c = remote(buf, slice(at[0], at[0] + 2 * rows), slice(at[1], at[1] + 2 * rows), cols, mate)
        c.start()
        return c

    def third(buf, fwd, cols):
        for q, f in fwd:
            if q == cols:
                f[0].wait_recv()
        return relay(buf, (0, 2), (1, 2), cols)

    def wait_all(*cs):
        for c in cs:
            c.wait_recv()

    xc, yc = _cols(XCH), _cols(YCH)

    def act(r):
        g0, g1 = _gelu(u_s[r, :].astype(BF16).astype(F32))
        z_ref[r, :] = g0.astype(BF16)
        u_s[r, :] = g1

    loc[0].wait()
    nx = [first(xg, c) for c in xc]
    px = relay(xg, (0, 0), (1, 0), slice(None))
    loc[1].wait()
    ny = [first(dyg, slice(yc[0].start, yc[0].stop)), first(dyg, slice(yc[1].start, yc[2].stop))]
    py = relay(dyg, (0, 0), (1, 0), slice(None))
    loc[2].start()
    loc[3].start()
    fx, rx = [], []
    for p, c in zip(nx, xc):
        fx += second(xg, p, (c,))
        rx.append(near(xg, c))
    loc[2].wait()
    wait_all(px, *rx)
    u_s[:most, :] = jnp.dot(xg[:most, :], w1_s[...], preferred_element_type=F32)
    fy = second(dyg, ny[0], yc[:1])

    @pl.loop(0, most // 16)
    def _(i):
        act(pl.ds(pl.multiple_of(i * 16, 16), 16))

    fy += second(dyg, ny[1], yc[1:], yc[2:])
    ry = near(dyg, slice(None))
    loc[3].wait()
    ox = [third(xg, fx, c) for c in xc]
    ox[0].wait_recv()
    u_s[most:, :] = jnp.dot(xg[most:, xc[0]], w1_s[xc[0], :], preferred_element_type=F32)
    oy = [third(dyg, fy, yc[0])]
    ox[1].wait_recv()
    u_s[most:, :] += jnp.dot(xg[most:, xc[1]], w1_s[xc[1], :], preferred_element_type=F32)
    oy.append(third(dyg, fy, yc[1]))
    wait_all(py, ry, oy[0])
    for i in range(most, n * rows, 16):
        act(slice(i, i + 16))
    g_s[...] = _nt(dyg[:, yc[0]], w2_s[:, yc[0]])
    wait_all(oy[1])
    g_s[...] += _nt(dyg[:, yc[1]], w2_s[:, yc[1]])
    for q, f in fy:
        if q == yc[2]:
            wait_all(*f)
    g = g_s[...] + _nt(dyg[:, yc[2]], w2_s[:, yc[2]])
    dz_ref[...] = (g * u_s[...]).astype(BF16)

    pcols = _cols(PCH)
    pc = []
    m = 3 * rows
    for j, cols in enumerate(pcols):
        part = _nt(dz_ref[...], w1_s[cols, :])
        psend[:m, cols] = part[m:2 * m].astype(BF16)
        psend[m:, cols] = part[2 * m + rows:].astype(BF16)
        c = pltpu.make_async_remote_copy(
            src_ref=psend.at[:, cols], dst_ref=precv.at[:, cols], send_sem=pss.at[j], recv_sem=prs.at[j],
            device_id={'tp': mate}, device_id_type=MESH)
        c.start()
        pc.append(c)
        keep_s[:m, cols] = part[:m]
        keep_s[m:, cols] = part[2 * m:2 * m + rows]
    for j, cols in enumerate(pcols):
        if j == len(pcols) - 1:
            for c in started:
                c.wait_send()
        pc[j].wait_recv()
        tot = [keep_s[d * rows:(d + 1) * rows, cols] + precv[d * rows:(d + 1) * rows, cols].astype(F32)
               for d in range(half)]
        own_ref[:, cols] = tot[0]
        plus_ref[:, cols] = tot[1].astype(BF16)
        minus_ref[:, cols] = tot[2].astype(BF16)
        opp_ref[:, cols] = tot[3].astype(BF16)
    for c in pc:
        c.wait_send()


def _hbm(*arrays):
    return [pltpu.with_memory_space_constraint(v, pltpu.MemorySpace.HBM) for v in arrays]


def _forward(x, dy, w1, w2, n):
    rows, hid = x.shape
    ff = w1.shape[1]
    t = rows * n
    vm = pl.BlockSpec(memory_space=pltpu.VMEM)
    hbm = pl.BlockSpec(memory_space=pltpu.MemorySpace.HBM)
    sd = jax.ShapeDtypeStruct
    dma = pltpu.SemaphoreType.DMA
    ncopies = 64
    return pl.pallas_call(
        functools.partial(_forward_kernel, n, rows),
        out_shape=(sd((t, hid), BF16), sd((t, hid), BF16), sd((t, ff), BF16), sd((t, ff), BF16),
                   sd((rows, hid), F32), sd((rows, hid), BF16), sd((rows, hid), BF16), sd((rows, hid), BF16)),
        in_specs=[hbm] * 4,
        out_specs=(vm,) * 8,
        scratch_shapes=[
            pltpu.VMEM((hid, ff), BF16), pltpu.VMEM((ff, hid), BF16),
            pltpu.VMEM((t, ff), F32), pltpu.VMEM((t, ff), F32),
            pltpu.VMEM((t // 2, hid), F32), pltpu.VMEM((t // 2, hid), BF16), pltpu.VMEM((t // 2, hid), BF16),
            dma((4,)), dma((ncopies,)), dma((ncopies,)), dma((len(PCH),)), dma((len(PCH),))],
        compiler_params=pltpu.CompilerParams(
            collective_id=0, has_side_effects=True, vmem_limit_bytes=36 << 20),
        name='gather_dz',
    )(*_hbm(x, dy, w1, w2))


def _wgrads(pairs, bm):
    def kernel(*refs):
        k = len(pairs)
        ins, outs, bufs, sem = refs[:2 * k], refs[2 * k:3 * k], refs[3 * k:4 * k], refs[4 * k]
        copies = []
        for p in range(k):
            a_ref, b_ref, o_ref, buf = ins[2 * p], ins[2 * p + 1], outs[p], bufs[p]
            for i in range(o_ref.shape[0] // bm):
                r = slice(i * bm, (i + 1) * bm)
                buf[r, :] = _tn(a_ref[:, r], b_ref[...])
                copies.append(pltpu.make_async_copy(buf.at[r], o_ref.at[r], sem.at[len(copies)]))
                copies[-1].start()
        for c in copies:
            c.wait()

    vm = pl.BlockSpec(memory_space=pltpu.VMEM)
    shapes = [(a.shape[1], b.shape[1]) for a, b in pairs]
    nsem = sum(s[0] // bm for s in shapes)
    t = pairs[0][0].shape[0]
    size = sum(s[0] * s[1] for s in shapes)
    return pl.pallas_call(
        kernel, out_shape=[jax.ShapeDtypeStruct(s, F32) for s in shapes], in_specs=[vm] * (2 * len(pairs)),
        out_specs=[pl.BlockSpec(memory_space=pltpu.MemorySpace.HBM)] * len(pairs), name='wgrads',
        scratch_shapes=[pltpu.VMEM(s, F32) for s in shapes] + [pltpu.SemaphoreType.DMA((nsem,))],
        compiler_params=pltpu.CompilerParams(vmem_limit_bytes=36 << 20),
        cost_estimate=pl.CostEstimate(flops=8 * t * size, bytes_accessed=4 * size, transcendentals=0),
    )(*[v for p in pairs for v in p])


def solution(mesh):
    n = mesh.shape['tp']
    half = n // 2

    def hop(v, d):
        return lax.ppermute(v, 'tp', [(2 * k + c, 2 * ((k + d) % half) + c) for k in range(half) for c in range(2)])

    def body(x, dy, w1, w2):
        xg, dyg, z, dz, own, plus, minus, opp = _forward(x, dy, w1, w2, n)
        parts = [hop(opp, 2), hop(plus, 1), hop(minus, half - 1)]
        dw2, dw1 = _wgrads([(z, dyg), (xg, dz)], 256)
        dx = own
        for p in parts:
            dx = dx + p.astype(F32)
        return dx.astype(BF16), dw1, dw2

    return jax.shard_map(
        body, mesh=mesh,
        in_specs=(P(('dp', 'tp'), None), P(('dp', 'tp'), None), P(None, 'tp'), P('tp', None)),
        out_specs=(P(('dp', 'tp'), None), P('dp', 'tp'), P(('dp', 'tp'), None)),
        check_vma=False)
```

```python
import functools
import math
import jax
import jax.numpy as jnp
from jax import lax
from jax.experimental import pallas as pl
from jax.experimental.pallas import tpu as pltpu
from jax.sharding import PartitionSpec as P

C0 = math.sqrt(2.0 / math.pi)
C1 = 0.044715
MESH = pl.DeviceIdType.MESH
F32, BF16 = jnp.float32, jnp.bfloat16
XCH = (1536, 1024)
YCH = (1024, 1024, 512)
PCH = (1536, 1024)
HEAD = 256
ORDER = ((0, 0), (0, 1), (0, 3), (1, 0), (1, 1), (1, 3), (0, 2), (1, 2))


def _gelu(u):
    q = (3.0 * C0 * C1 * u) * u
    t = jnp.tanh(u * (C0 + q * (1.0 / 3.0)))
    p = 0.5 + 0.5 * t
    z = u * p
    return z, p + (z * (1.0 - t)) * (C0 + q)


def _nt(a, b):
    return lax.dot_general(a, b, (((1,), (1,)), ((), ())), preferred_element_type=F32)


def _tn(a, b):
    return lax.dot_general(a, b, (((0,), (0,)), ((), ())), preferred_element_type=F32)


def _cols(sizes, at=0):
    out = []
    for s in sizes:
        out.append(slice(at, at + s))
        at += s
    return out


def _forward_kernel(n, rows,
                    x_ref, dy_ref, w1_ref, w2_ref,
                    xg, dyg, z_ref, dz_ref, own_ref, plus_ref, minus_ref, opp_ref, head_ref,
                    w1_s, w2_s, u_s, g_s, keep_s, psend, precv,
                    lsem, ssem, rsem, pss, prs):
    half = n // 2
    me = lax.axis_index('tp')
    chip, core = me // 2, me % 2
    right = ((chip + 1) % half) * 2 + core
    left = ((chip + half - 1) % half) * 2 + core
    mate = chip * 2 + (1 - core)
    h = rows // 2
    most = (n - 2) * rows

    def blk(s, d, lo=0, size=rows):
        at = ORDER.index((s, d)) * rows + lo
        return slice(at, at + size)

    loc = [pltpu.make_async_copy(x_ref, xg.at[blk(0, 0)], lsem.at[0]),
           pltpu.make_async_copy(dy_ref, dyg.at[blk(0, 0)], lsem.at[1]),
           pltpu.make_async_copy(w1_ref, w1_s, lsem.at[2]),
           pltpu.make_async_copy(w2_ref, w2_s, lsem.at[3])]
    loc[0].start()
    loc[1].start()

    barrier = pltpu.get_barrier_semaphore()
    for peer in (mate, left, right):
        pl.semaphore_signal(barrier, inc=1, device_id={'tp': peer}, device_id_type=MESH)
    pl.semaphore_wait(barrier, 3)

    used = [0]
    started = []

    def remote(buf, src, dst, cols, dev):
        i = used[0]
        used[0] += 1
        c = pltpu.make_async_remote_copy(
            src_ref=buf.at[src, cols], dst_ref=buf.at[dst, cols], send_sem=ssem.at[i], recv_sem=rsem.at[i],
            device_id={'tp': dev}, device_id_type=MESH)
        started.append(c)
        return c

    def first(buf, cols):
        a = remote(buf, blk(0, 0), blk(0, 3), cols, right)
        b = remote(buf, blk(0, 0), blk(0, 1), cols, left)
        a.start()
        b.start()
        return a, b

    def relay(buf, src, dst, cols):
        c = remote(buf, blk(*src), blk(*dst), cols, mate)
        c.start()
        return c

    def second(buf, pair, parts, both=()):
        out = []
        for k, (c, s, d, lo, dev, dev2) in enumerate((
                (pair[0], (0, 3), (0, 2), 0, right, right + 1 - 2 * core),
                (pair[1], (0, 1), (0, 2), h, left, left + 1 - 2 * core))):
            c.wait_recv()
            for q in parts:
                f = [remote(buf, blk(*s, lo, h), blk(*d, lo, h), q, dev)]
                if q in both:
                    f.append(remote(buf, blk(*s, lo, h), blk(1, 2, lo, h), q, dev2))
                for v in f:
                    v.start()
                out.append((q, f))
        return out

    def near(buf, cols):
        at = blk(0, 1).start, blk(1, 1).start
        c = remote(buf, slice(at[0], at[0] + 2 * rows), slice(at[1], at[1] + 2 * rows), cols, mate)
        c.start()
        return c

    def third(buf, fwd, cols):
        for q, f in fwd:
            if q == cols:
                f[0].wait_recv()
        return relay(buf, (0, 2), (1, 2), cols)

    def wait_all(*cs):
        for c in cs:
            c.wait_recv()

    xc, yc = _cols(XCH), _cols(YCH)

    def act(r):
        g0, g1 = _gelu(u_s[r, :].astype(BF16).astype(F32))
        z_ref[r, :] = g0.astype(BF16)
        u_s[r, :] = g1

    loc[0].wait()
    nx = [first(xg, c) for c in xc]
    px = relay(xg, (0, 0), (1, 0), slice(None))
    loc[1].wait()
    ny = [first(dyg, slice(yc[0].start, yc[0].stop)), first(dyg, slice(yc[1].start, yc[2].stop))]
    py = relay(dyg, (0, 0), (1, 0), slice(None))
    loc[2].start()
    loc[3].start()
    fx, rx = [], []
    for p, c in zip(nx, xc):
        fx += second(xg, p, (c,))
        rx.append(near(xg, c))
    loc[2].wait()
    wait_all(px, *rx)
    u_s[:most, :] = jnp.dot(xg[:most, :], w1_s[...], preferred_element_type=F32)
    fy = second(dyg, ny[0], yc[:1])

    @pl.loop(0, most // 16)
    def _(i):
        act(pl.ds(pl.multiple_of(i * 16, 16), 16))

    fy += second(dyg, ny[1], yc[1:], yc[2:])
    ry = near(dyg, slice(None))
    loc[3].wait()
    ox = [third(xg, fx, c) for c in xc]
    ox[0].wait_recv()
    u_s[most:, :] = jnp.dot(xg[most:, xc[0]], w1_s[xc[0], :], preferred_element_type=F32)
    oy = [third(dyg, fy, yc[0])]
    ox[1].wait_recv()
    u_s[most:, :] += jnp.dot(xg[most:, xc[1]], w1_s[xc[1], :], preferred_element_type=F32)
    oy.append(third(dyg, fy, yc[1]))
    wait_all(py, ry, oy[0])
    for i in range(most, n * rows, 16):
        act(slice(i, i + 16))
    g_s[...] = _nt(dyg[:, yc[0]], w2_s[:, yc[0]])
    wait_all(oy[1])
    g_s[...] += _nt(dyg[:, yc[1]], w2_s[:, yc[1]])
    for q, f in fy:
        if q == yc[2]:
            wait_all(*f)
    g = g_s[...] + _nt(dyg[:, yc[2]], w2_s[:, yc[2]])
    dz_ref[...] = (g * u_s[...]).astype(BF16)

    pcols = _cols(PCH)
    pc = []
    m = 3 * rows
    for j, cols in enumerate(pcols):
        part = _nt(dz_ref[...], w1_s[cols, :])
        psend[:m, cols] = part[m:2 * m].astype(BF16)
        psend[m:, cols] = part[2 * m + rows:].astype(BF16)
        c = pltpu.make_async_remote_copy(
            src_ref=psend.at[:, cols], dst_ref=precv.at[:, cols], send_sem=pss.at[j], recv_sem=prs.at[j],
            device_id={'tp': mate}, device_id_type=MESH)
        c.start()
        pc.append(c)
        keep_s[:m, cols] = part[:m]
        keep_s[m:, cols] = part[2 * m:2 * m + rows]
    head_ref[...] = _tn(z_ref[:, :HEAD], dyg[...])
    for j, cols in enumerate(pcols):
        if j == len(pcols) - 1:
            for c in started:
                c.wait_send()
        pc[j].wait_recv()
        tot = [keep_s[d * rows:(d + 1) * rows, cols] + precv[d * rows:(d + 1) * rows, cols].astype(F32)
               for d in range(half)]
        own_ref[:, cols] = tot[0]
        plus_ref[:, cols] = tot[1].astype(BF16)
        minus_ref[:, cols] = tot[2].astype(BF16)
        opp_ref[:, cols] = tot[3].astype(BF16)
    for c in pc:
        c.wait_send()


def _hbm(*arrays):
    return [pltpu.with_memory_space_constraint(v, pltpu.MemorySpace.HBM) for v in arrays]


def _forward(x, dy, w1, w2, n):
    rows, hid = x.shape
    ff = w1.shape[1]
    t = rows * n
    vm = pl.BlockSpec(memory_space=pltpu.VMEM)
    hbm = pl.BlockSpec(memory_space=pltpu.MemorySpace.HBM)
    sd = jax.ShapeDtypeStruct
    dma = pltpu.SemaphoreType.DMA
    ncopies = 64
    return pl.pallas_call(
        functools.partial(_forward_kernel, n, rows),
        out_shape=(sd((t, hid), BF16), sd((t, hid), BF16), sd((t, ff), BF16), sd((t, ff), BF16),
                   sd((rows, hid), F32), sd((rows, hid), BF16), sd((rows, hid), BF16), sd((rows, hid), BF16),
                   sd((HEAD, hid), F32)),
        in_specs=[hbm] * 4,
        out_specs=(vm,) * 9,
        scratch_shapes=[
            pltpu.VMEM((hid, ff), BF16), pltpu.VMEM((ff, hid), BF16),
            pltpu.VMEM((t, ff), F32), pltpu.VMEM((t, ff), F32),
            pltpu.VMEM((t // 2, hid), F32), pltpu.VMEM((t // 2, hid), BF16), pltpu.VMEM((t // 2, hid), BF16),
            dma((4,)), dma((ncopies,)), dma((ncopies,)), dma((len(PCH),)), dma((len(PCH),))],
        compiler_params=pltpu.CompilerParams(
            collective_id=0, has_side_effects=True, vmem_limit_bytes=36 << 20),
        name='gather_dz',
    )(*_hbm(x, dy, w1, w2))


def _wgrads(head, pairs, bm):
    k = len(pairs)
    shapes = [(a.shape[1], b.shape[1]) for a, b in pairs]
    skip = [head.shape[0]] + [0] * (k - 1)

    def kernel(head_ref, *refs):
        ins, outs, bufs, sem = refs[:2 * k], refs[2 * k:3 * k], refs[3 * k:4 * k], refs[4 * k]
        copies = [pltpu.make_async_copy(head_ref, outs[0].at[:skip[0]], sem.at[0])]
        copies[0].start()
        for p in range(k):
            a_ref, b_ref, o_ref, buf = ins[2 * p], ins[2 * p + 1], outs[p], bufs[p]
            for i in range(skip[p], shapes[p][0], bm):
                r, w = slice(i, i + bm), slice(i - skip[p], i - skip[p] + bm)
                buf[w, :] = _tn(a_ref[:, r], b_ref[...])
                copies.append(pltpu.make_async_copy(buf.at[w], o_ref.at[r], sem.at[len(copies)]))
                copies[-1].start()
        for c in copies:
            c.wait()

    vm = pl.BlockSpec(memory_space=pltpu.VMEM)
    nsem = 1 + sum((s[0] - d) // bm for s, d in zip(shapes, skip))
    t = pairs[0][0].shape[0]
    size = sum(s[0] * s[1] for s in shapes)
    return pl.pallas_call(
        kernel, out_shape=[jax.ShapeDtypeStruct(s, F32) for s in shapes], in_specs=[vm] * (2 * k + 1),
        out_specs=[pl.BlockSpec(memory_space=pltpu.MemorySpace.HBM)] * k, name='wgrads',
        scratch_shapes=[pltpu.VMEM((s[0] - d, s[1]), F32) for s, d in zip(shapes, skip)]
        + [pltpu.SemaphoreType.DMA((nsem,))],
        compiler_params=pltpu.CompilerParams(vmem_limit_bytes=36 << 20),
        cost_estimate=pl.CostEstimate(flops=8 * t * size, bytes_accessed=4 * size, transcendentals=0),
    )(head, *[v for p in pairs for v in p])


def solution(mesh):
    n = mesh.shape['tp']
    half = n // 2

    def hop(v, d):
        return lax.ppermute(v, 'tp', [(2 * k + c, 2 * ((k + d) % half) + c) for k in range(half) for c in range(2)])

    def body(x, dy, w1, w2):
        xg, dyg, z, dz, own, plus, minus, opp, head = _forward(x, dy, w1, w2, n)
        parts = [hop(opp, 2), hop(plus, 1), hop(minus, half - 1)]
        dw2, dw1 = _wgrads(head, [(z, dyg), (xg, dz)], 256)
        dx = own
        for p in parts:
            dx = dx + p.astype(F32)
        return dx.astype(BF16), dw1, dw2

    return jax.shard_map(
        body, mesh=mesh,
        in_specs=(P(('dp', 'tp'), None), P(('dp', 'tp'), None), P(None, 'tp'), P('tp', None)),
        out_specs=(P(('dp', 'tp'), None), P('dp', 'tp'), P(('dp', 'tp'), None)),
        check_vma=False)
```

```python
import functools
import math
import jax
import jax.numpy as jnp
from jax import lax
from jax.experimental import pallas as pl
from jax.experimental.pallas import tpu as pltpu
from jax.sharding import PartitionSpec as P

C0 = math.sqrt(2.0 / math.pi)
C1 = 0.044715
MESH = pl.DeviceIdType.MESH
F32, BF16 = jnp.float32, jnp.bfloat16
XCH = (1536, 1024)
YCH = (1024, 768, 768)
PCH = (1536, 1024)
HEAD = 256
ORDER = ((0, 0), (0, 1), (0, 3), (1, 0), (1, 1), (1, 3), (0, 2), (1, 2))


def _gelu(u):
    q = (3.0 * C0 * C1 * u) * u
    t = jnp.tanh(u * (C0 + q * (1.0 / 3.0)))
    p = 0.5 + 0.5 * t
    z = u * p
    return z, p + (z * (1.0 - t)) * (C0 + q)


def _nt(a, b):
    return lax.dot_general(a, b, (((1,), (1,)), ((), ())), preferred_element_type=F32)


def _tn(a, b):
    return lax.dot_general(a, b, (((0,), (0,)), ((), ())), preferred_element_type=F32)


def _cols(sizes, at=0):
    out = []
    for s in sizes:
        out.append(slice(at, at + s))
        at += s
    return out


def _forward_kernel(n, rows,
                    x_ref, dy_ref, w1_ref, w2_ref,
                    xg, dyg, z_ref, dz_ref, own_ref, plus_ref, minus_ref, opp_ref, head_ref,
                    w1_s, w2_s, u_s, g_s, keep_s, psend, precv,
                    lsem, ssem, rsem, pss, prs):
    half = n // 2
    me = lax.axis_index('tp')
    chip, core = me // 2, me % 2
    right = ((chip + 1) % half) * 2 + core
    left = ((chip + half - 1) % half) * 2 + core
    mate = chip * 2 + (1 - core)
    h = rows // 2
    most = (n - 2) * rows

    def blk(s, d, lo=0, size=rows):
        at = ORDER.index((s, d)) * rows + lo
        return slice(at, at + size)

    loc = [pltpu.make_async_copy(x_ref, xg.at[blk(0, 0)], lsem.at[0]),
           pltpu.make_async_copy(dy_ref, dyg.at[blk(0, 0)], lsem.at[1]),
           pltpu.make_async_copy(w1_ref, w1_s, lsem.at[2]),
           pltpu.make_async_copy(w2_ref, w2_s, lsem.at[3])]
    loc[0].start()
    loc[1].start()

    barrier = pltpu.get_barrier_semaphore()
    for peer in (mate, left, right):
        pl.semaphore_signal(barrier, inc=1, device_id={'tp': peer}, device_id_type=MESH)
    pl.semaphore_wait(barrier, 3)

    used = [0]
    started = []

    def remote(buf, src, dst, cols, dev):
        i = used[0]
        used[0] += 1
        c = pltpu.make_async_remote_copy(
            src_ref=buf.at[src, cols], dst_ref=buf.at[dst, cols], send_sem=ssem.at[i], recv_sem=rsem.at[i],
            device_id={'tp': dev}, device_id_type=MESH)
        started.append(c)
        return c

    def first(buf, cols):
        a = remote(buf, blk(0, 0), blk(0, 3), cols, right)
        b = remote(buf, blk(0, 0), blk(0, 1), cols, left)
        a.start()
        b.start()
        return a, b

    def relay(buf, src, dst, cols):
        c = remote(buf, blk(*src), blk(*dst), cols, mate)
        c.start()
        return c

    def second(buf, pair, parts, both=()):
        out = []
        for k, (c, s, d, lo, dev, dev2) in enumerate((
                (pair[0], (0, 3), (0, 2), 0, right, right + 1 - 2 * core),
                (pair[1], (0, 1), (0, 2), h, left, left + 1 - 2 * core))):
            c.wait_recv()
            for q in parts:
                f = [remote(buf, blk(*s, lo, h), blk(*d, lo, h), q, dev)]
                if q in both:
                    f.append(remote(buf, blk(*s, lo, h), blk(1, 2, lo, h), q, dev2))
                for v in f:
                    v.start()
                out.append((q, f))
        return out

    def near(buf, cols):
        at = blk(0, 1).start, blk(1, 1).start
        c = remote(buf, slice(at[0], at[0] + 2 * rows), slice(at[1], at[1] + 2 * rows), cols, mate)
        c.start()
        return c

    def third(buf, fwd, cols):
        for q, f in fwd:
            if q == cols:
                f[0].wait_recv()
        return relay(buf, (0, 2), (1, 2), cols)

    def wait_all(*cs):
        for c in cs:
            c.wait_recv()

    xc, yc = _cols(XCH), _cols(YCH)

    def act(r):
        g0, g1 = _gelu(u_s[r, :].astype(BF16).astype(F32))
        z_ref[r, :] = g0.astype(BF16)
        u_s[r, :] = g1

    loc[0].wait()
    nx = [first(xg, c) for c in xc]
    px = relay(xg, (0, 0), (1, 0), slice(None))
    loc[1].wait()
    ny = [first(dyg, slice(yc[0].start, yc[0].stop)), first(dyg, slice(yc[1].start, yc[2].stop))]
    py = relay(dyg, (0, 0), (1, 0), slice(None))
    loc[2].start()
    loc[3].start()
    fx, rx = [], []
    for p, c in zip(nx, xc):
        fx += second(xg, p, (c,))
        rx.append(near(xg, c))
    loc[2].wait()
    wait_all(px, *rx)
    u_s[:most, :] = jnp.dot(xg[:most, :], w1_s[...], preferred_element_type=F32)
    fy = second(dyg, ny[0], yc[:1])

    @pl.loop(0, most // 16)
    def _(i):
        act(pl.ds(pl.multiple_of(i * 16, 16), 16))

    fy += second(dyg, ny[1], yc[1:], yc[2:])
    ry = near(dyg, slice(None))
    loc[3].wait()
    ox = [third(xg, fx, c) for c in xc]
    ox[0].wait_recv()
    u_s[most:, :] = jnp.dot(xg[most:, xc[0]], w1_s[xc[0], :], preferred_element_type=F32)
    oy = [third(dyg, fy, yc[0])]
    ox[1].wait_recv()
    u_s[most:, :] += jnp.dot(xg[most:, xc[1]], w1_s[xc[1], :], preferred_element_type=F32)
    oy.append(third(dyg, fy, yc[1]))
    wait_all(py, ry, oy[0])
    for i in range(most, n * rows, 16):
        act(slice(i, i + 16))
    g_s[...] = _nt(dyg[:, yc[0]], w2_s[:, yc[0]])
    wait_all(oy[1])
    g_s[...] += _nt(dyg[:, yc[1]], w2_s[:, yc[1]])
    for q, f in fy:
        if q == yc[2]:
            wait_all(*f)
    g = g_s[...] + _nt(dyg[:, yc[2]], w2_s[:, yc[2]])
    dz_ref[...] = (g * u_s[...]).astype(BF16)

    pcols = _cols(PCH)
    pc = []
    m = 3 * rows
    for j, cols in enumerate(pcols):
        part = _nt(dz_ref[...], w1_s[cols, :])
        psend[:m, cols] = part[m:2 * m].astype(BF16)
        psend[m:, cols] = part[2 * m + rows:].astype(BF16)
        c = pltpu.make_async_remote_copy(
            src_ref=psend.at[:, cols], dst_ref=precv.at[:, cols], send_sem=pss.at[j], recv_sem=prs.at[j],
            device_id={'tp': mate}, device_id_type=MESH)
        c.start()
        pc.append(c)
        keep_s[:m, cols] = part[:m]
        keep_s[m:, cols] = part[2 * m:2 * m + rows]
    head_ref[...] = _tn(z_ref[:, :HEAD], dyg[...])
    for j, cols in enumerate(pcols):
        if j == len(pcols) - 1:
            for c in started:
                c.wait_send()
        pc[j].wait_recv()
        tot = [keep_s[d * rows:(d + 1) * rows, cols] + precv[d * rows:(d + 1) * rows, cols].astype(F32)
               for d in range(half)]
        own_ref[:, cols] = tot[0]
        plus_ref[:, cols] = tot[1].astype(BF16)
        minus_ref[:, cols] = tot[2].astype(BF16)
        opp_ref[:, cols] = tot[3].astype(BF16)
    for c in pc:
        c.wait_send()


def _hbm(*arrays):
    return [pltpu.with_memory_space_constraint(v, pltpu.MemorySpace.HBM) for v in arrays]


def _forward(x, dy, w1, w2, n):
    rows, hid = x.shape
    ff = w1.shape[1]
    t = rows * n
    vm = pl.BlockSpec(memory_space=pltpu.VMEM)
    hbm = pl.BlockSpec(memory_space=pltpu.MemorySpace.HBM)
    sd = jax.ShapeDtypeStruct
    dma = pltpu.SemaphoreType.DMA
    ncopies = 64
    return pl.pallas_call(
        functools.partial(_forward_kernel, n, rows),
        out_shape=(sd((t, hid), BF16), sd((t, hid), BF16), sd((t, ff), BF16), sd((t, ff), BF16),
                   sd((rows, hid), F32), sd((rows, hid), BF16), sd((rows, hid), BF16), sd((rows, hid), BF16),
                   sd((HEAD, hid), F32)),
        in_specs=[hbm] * 4,
        out_specs=(vm,) * 9,
        scratch_shapes=[
            pltpu.VMEM((hid, ff), BF16), pltpu.VMEM((ff, hid), BF16),
            pltpu.VMEM((t, ff), F32), pltpu.VMEM((t, ff), F32),
            pltpu.VMEM((t // 2, hid), F32), pltpu.VMEM((t // 2, hid), BF16), pltpu.VMEM((t // 2, hid), BF16),
            dma((4,)), dma((ncopies,)), dma((ncopies,)), dma((len(PCH),)), dma((len(PCH),))],
        compiler_params=pltpu.CompilerParams(
            collective_id=0, has_side_effects=True, vmem_limit_bytes=36 << 20),
        name='gather_dz',
    )(*_hbm(x, dy, w1, w2))


def _wgrads(head, pairs, bm):
    k = len(pairs)
    shapes = [(a.shape[1], b.shape[1]) for a, b in pairs]
    skip = [head.shape[0]] + [0] * (k - 1)

    def kernel(head_ref, *refs):
        ins, outs, bufs, sem = refs[:2 * k], refs[2 * k:3 * k], refs[3 * k:4 * k], refs[4 * k]
        copies = [pltpu.make_async_copy(head_ref, outs[0].at[:skip[0]], sem.at[0])]
        copies[0].start()
        for p in range(k):
            a_ref, b_ref, o_ref, buf = ins[2 * p], ins[2 * p + 1], outs[p], bufs[p]
            for i in range(skip[p], shapes[p][0], bm):
                r, w = slice(i, i + bm), slice(i - skip[p], i - skip[p] + bm)
                buf[w, :] = _tn(a_ref[:, r], b_ref[...])
                copies.append(pltpu.make_async_copy(buf.at[w], o_ref.at[r], sem.at[len(copies)]))
                copies[-1].start()
        for c in copies:
            c.wait()

    vm = pl.BlockSpec(memory_space=pltpu.VMEM)
    nsem = 1 + sum((s[0] - d) // bm for s, d in zip(shapes, skip))
    t = pairs[0][0].shape[0]
    size = sum(s[0] * s[1] for s in shapes)
    return pl.pallas_call(
        kernel, out_shape=[jax.ShapeDtypeStruct(s, F32) for s in shapes], in_specs=[vm] * (2 * k + 1),
        out_specs=[pl.BlockSpec(memory_space=pltpu.MemorySpace.HBM)] * k, name='wgrads',
        scratch_shapes=[pltpu.VMEM((s[0] - d, s[1]), F32) for s, d in zip(shapes, skip)]
        + [pltpu.SemaphoreType.DMA((nsem,))],
        compiler_params=pltpu.CompilerParams(vmem_limit_bytes=36 << 20),
        cost_estimate=pl.CostEstimate(flops=8 * t * size, bytes_accessed=4 * size, transcendentals=0),
    )(head, *[v for p in pairs for v in p])


def solution(mesh):
    n = mesh.shape['tp']
    half = n // 2

    def hop(v, d):
        return lax.ppermute(v, 'tp', [(2 * k + c, 2 * ((k + d) % half) + c) for k in range(half) for c in range(2)])

    def body(x, dy, w1, w2):
        xg, dyg, z, dz, own, plus, minus, opp, head = _forward(x, dy, w1, w2, n)
        parts = [hop(plus, 1), hop(minus, half - 1), hop(opp, 2)]
        dw2, dw1 = _wgrads(head, [(z, dyg), (xg, dz)], 256)
        dx = own
        for p in parts:
            dx = dx + p.astype(F32)
        return dx.astype(BF16), dw1, dw2

    return jax.shard_map(
        body, mesh=mesh,
        in_specs=(P(('dp', 'tp'), None), P(('dp', 'tp'), None), P(None, 'tp'), P('tp', None)),
        out_specs=(P(('dp', 'tp'), None), P('dp', 'tp'), P(('dp', 'tp'), None)),
        check_vma=False)
```

```python
import functools
import math
import jax
import jax.numpy as jnp
from jax import lax
from jax.experimental import pallas as pl
from jax.experimental.pallas import tpu as pltpu
from jax.sharding import PartitionSpec as P

C0 = math.sqrt(2.0 / math.pi)
C1 = 0.044715
MESH = pl.DeviceIdType.MESH
F32, BF16 = jnp.float32, jnp.bfloat16
XCH = (1536, 1024)
YCH = (1024, 768, 768)
PCH = (1536, 1024)
HEAD = 256
ORDER = ((0, 0), (0, 1), (0, 3), (1, 0), (1, 1), (1, 3), (0, 2), (1, 2))


def _gelu(u):
    q = (3.0 * C0 * C1 * u) * u
    t = jnp.tanh(u * (C0 + q * (1.0 / 3.0)))
    p = 0.5 + 0.5 * t
    z = u * p
    return z, p + (z * (1.0 - t)) * (C0 + q)


def _nt(a, b):
    return lax.dot_general(a, b, (((1,), (1,)), ((), ())), preferred_element_type=F32)


def _tn(a, b):
    return lax.dot_general(a, b, (((0,), (0,)), ((), ())), preferred_element_type=F32)


def _cols(sizes, at=0):
    out = []
    for s in sizes:
        out.append(slice(at, at + s))
        at += s
    return out


def _forward_kernel(n, rows,
                    x_ref, dy_ref, w1_ref, w2_ref,
                    xg, dyg, z_ref, dz_ref, own_ref, plus_ref, minus_ref, opp_ref, head_ref,
                    w1_s, w2_s, u_s, g_s, keep_s, psend, precv,
                    lsem, ssem, rsem, pss, prs):
    half = n // 2
    me = lax.axis_index('tp')
    chip, core = me // 2, me % 2
    right = ((chip + 1) % half) * 2 + core
    left = ((chip + half - 1) % half) * 2 + core
    mate = chip * 2 + (1 - core)
    h = rows // 2
    most = (n - 2) * rows

    def blk(s, d, lo=0, size=rows):
        at = ORDER.index((s, d)) * rows + lo
        return slice(at, at + size)

    loc = [pltpu.make_async_copy(x_ref, xg.at[blk(0, 0)], lsem.at[0]),
           pltpu.make_async_copy(dy_ref, dyg.at[blk(0, 0)], lsem.at[1]),
           pltpu.make_async_copy(w1_ref, w1_s, lsem.at[2]),
           pltpu.make_async_copy(w2_ref, w2_s, lsem.at[3])]
    loc[0].start()
    loc[1].start()

    barrier = pltpu.get_barrier_semaphore()
    for peer in (mate, left, right):
        pl.semaphore_signal(barrier, inc=1, device_id={'tp': peer}, device_id_type=MESH)
    pl.semaphore_wait(barrier, 3)

    used = [0]
    started = []

    def remote(buf, src, dst, cols, dev):
        i = used[0]
        used[0] += 1
        c = pltpu.make_async_remote_copy(
            src_ref=buf.at[src, cols], dst_ref=buf.at[dst, cols], send_sem=ssem.at[i], recv_sem=rsem.at[i],
            device_id={'tp': dev}, device_id_type=MESH)
        started.append(c)
        return c

    def first(buf, cols):
        a = remote(buf, blk(0, 0), blk(0, 3), cols, right)
        b = remote(buf, blk(0, 0), blk(0, 1), cols, left)
        a.start()
        b.start()
        return a, b

    def relay(buf, src, dst, cols):
        c = remote(buf, blk(*src), blk(*dst), cols, mate)
        c.start()
        return c

    def second(buf, pair, parts, both=()):
        out = []
        for k, (c, s, d, lo, dev, dev2) in enumerate((
                (pair[0], (0, 3), (0, 2), 0, right, right + 1 - 2 * core),
                (pair[1], (0, 1), (0, 2), h, left, left + 1 - 2 * core))):
            c.wait_recv()
            for q in parts:
                f = [remote(buf, blk(*s, lo, h), blk(*d, lo, h), q, dev)]
                if q in both:
                    f.append(remote(buf, blk(*s, lo, h), blk(1, 2, lo, h), q, dev2))
                for v in f:
                    v.start()
                out.append((q, f))
        return out

    def near(buf, cols):
        at = blk(0, 1).start, blk(1, 1).start
        c = remote(buf, slice(at[0], at[0] + 2 * rows), slice(at[1], at[1] + 2 * rows), cols, mate)
        c.start()
        return c

    def third(buf, fwd, cols):
        for q, f in fwd:
            if q == cols:
                f[0].wait_recv()
        return relay(buf, (0, 2), (1, 2), cols)

    def wait_all(*cs):
        for c in cs:
            c.wait_recv()

    xc, yc = _cols(XCH), _cols(YCH)

    def act(r):
        g0, g1 = _gelu(u_s[r, :].astype(BF16).astype(F32))
        z_ref[r, :] = g0.astype(BF16)
        u_s[r, :] = g1

    loc[0].wait()
    nx = [first(xg, c) for c in xc]
    px = relay(xg, (0, 0), (1, 0), slice(None))
    loc[1].wait()
    ny = [first(dyg, slice(yc[0].start, yc[0].stop)), first(dyg, slice(yc[1].start, yc[2].stop))]
    py = relay(dyg, (0, 0), (1, 0), slice(None))
    loc[2].start()
    loc[3].start()
    fx, rx = [], []
    for p, c in zip(nx, xc):
        fx += second(xg, p, (c,))
        rx.append(near(xg, c))
    loc[2].wait()
    wait_all(px, *rx)
    u_s[:most, :] = jnp.dot(xg[:most, :], w1_s[...], preferred_element_type=F32)
    fy = second(dyg, ny[0], yc[:1])

    @pl.loop(0, most // 16)
    def _(i):
        act(pl.ds(pl.multiple_of(i * 16, 16), 16))

    fy += second(dyg, ny[1], yc[1:], yc[1:])
    ry = near(dyg, slice(None))
    loc[3].wait()
    ox = [third(xg, fx, c) for c in xc]
    ox[0].wait_recv()
    u_s[most:, :] = jnp.dot(xg[most:, xc[0]], w1_s[xc[0], :], preferred_element_type=F32)
    oy = [third(dyg, fy, yc[0])]
    ox[1].wait_recv()
    u_s[most:, :] += jnp.dot(xg[most:, xc[1]], w1_s[xc[1], :], preferred_element_type=F32)
    wait_all(py, ry, oy[0])
    for i in range(most, n * rows, 16):
        act(slice(i, i + 16))
    g_s[...] = _nt(dyg[:, yc[0]], w2_s[:, yc[0]])
    for q, f in fy:
        if q == yc[1]:
            wait_all(*f)
    g_s[...] += _nt(dyg[:, yc[1]], w2_s[:, yc[1]])
    for q, f in fy:
        if q == yc[2]:
            wait_all(*f)
    g = g_s[...] + _nt(dyg[:, yc[2]], w2_s[:, yc[2]])
    dz_ref[...] = (g * u_s[...]).astype(BF16)

    pcols = _cols(PCH)
    pc = []
    m = 3 * rows
    for j, cols in enumerate(pcols):
        part = _nt(dz_ref[...], w1_s[cols, :])
        psend[:m, cols] = part[m:2 * m].astype(BF16)
        psend[m:, cols] = part[2 * m + rows:].astype(BF16)
        c = pltpu.make_async_remote_copy(
            src_ref=psend.at[:, cols], dst_ref=precv.at[:, cols], send_sem=pss.at[j], recv_sem=prs.at[j],
            device_id={'tp': mate}, device_id_type=MESH)
        c.start()
        pc.append(c)
        keep_s[:m, cols] = part[:m]
        keep_s[m:, cols] = part[2 * m:2 * m + rows]
    head_ref[...] = _tn(z_ref[:, :HEAD], dyg[...])
    for j, cols in enumerate(pcols):
        if j == len(pcols) - 1:
            for c in started:
                c.wait_send()
        pc[j].wait_recv()
        tot = [keep_s[d * rows:(d + 1) * rows, cols] + precv[d * rows:(d + 1) * rows, cols].astype(F32)
               for d in range(half)]
        own_ref[:, cols] = tot[0]
        plus_ref[:, cols] = tot[1].astype(BF16)
        minus_ref[:, cols] = tot[2].astype(BF16)
        opp_ref[:, cols] = tot[3].astype(BF16)
    for c in pc:
        c.wait_send()


def _hbm(*arrays):
    return [pltpu.with_memory_space_constraint(v, pltpu.MemorySpace.HBM) for v in arrays]


def _forward(x, dy, w1, w2, n):
    rows, hid = x.shape
    ff = w1.shape[1]
    t = rows * n
    vm = pl.BlockSpec(memory_space=pltpu.VMEM)
    hbm = pl.BlockSpec(memory_space=pltpu.MemorySpace.HBM)
    sd = jax.ShapeDtypeStruct
    dma = pltpu.SemaphoreType.DMA
    ncopies = 64
    return pl.pallas_call(
        functools.partial(_forward_kernel, n, rows),
        out_shape=(sd((t, hid), BF16), sd((t, hid), BF16), sd((t, ff), BF16), sd((t, ff), BF16),
                   sd((rows, hid), F32), sd((rows, hid), BF16), sd((rows, hid), BF16), sd((rows, hid), BF16),
                   sd((HEAD, hid), F32)),
        in_specs=[hbm] * 4,
        out_specs=(vm,) * 9,
        scratch_shapes=[
            pltpu.VMEM((hid, ff), BF16), pltpu.VMEM((ff, hid), BF16),
            pltpu.VMEM((t, ff), F32), pltpu.VMEM((t, ff), F32),
            pltpu.VMEM((t // 2, hid), F32), pltpu.VMEM((t // 2, hid), BF16), pltpu.VMEM((t // 2, hid), BF16),
            dma((4,)), dma((ncopies,)), dma((ncopies,)), dma((len(PCH),)), dma((len(PCH),))],
        compiler_params=pltpu.CompilerParams(
            collective_id=0, has_side_effects=True, vmem_limit_bytes=36 << 20),
        name='gather_dz',
    )(*_hbm(x, dy, w1, w2))


def _wgrads(head, pairs, bm):
    k = len(pairs)
    shapes = [(a.shape[1], b.shape[1]) for a, b in pairs]
    skip = [head.shape[0]] + [0] * (k - 1)

    def kernel(head_ref, *refs):
        ins, outs, bufs, sem = refs[:2 * k], refs[2 * k:3 * k], refs[3 * k:4 * k], refs[4 * k]
        copies = [pltpu.make_async_copy(head_ref, outs[0].at[:skip[0]], sem.at[0])]
        copies[0].start()
        for p in range(k):
            a_ref, b_ref, o_ref, buf = ins[2 * p], ins[2 * p + 1], outs[p], bufs[p]
            for i in range(skip[p], shapes[p][0], bm):
                r, w = slice(i, i + bm), slice(i - skip[p], i - skip[p] + bm)
                buf[w, :] = _tn(a_ref[:, r], b_ref[...])
                copies.append(pltpu.make_async_copy(buf.at[w], o_ref.at[r], sem.at[len(copies)]))
                copies[-1].start()
        for c in copies:
            c.wait()

    vm = pl.BlockSpec(memory_space=pltpu.VMEM)
    nsem = 1 + sum((s[0] - d) // bm for s, d in zip(shapes, skip))
    t = pairs[0][0].shape[0]
    size = sum(s[0] * s[1] for s in shapes)
    return pl.pallas_call(
        kernel, out_shape=[jax.ShapeDtypeStruct(s, F32) for s in shapes], in_specs=[vm] * (2 * k + 1),
        out_specs=[pl.BlockSpec(memory_space=pltpu.MemorySpace.HBM)] * k, name='wgrads',
        scratch_shapes=[pltpu.VMEM((s[0] - d, s[1]), F32) for s, d in zip(shapes, skip)]
        + [pltpu.SemaphoreType.DMA((nsem,))],
        compiler_params=pltpu.CompilerParams(vmem_limit_bytes=36 << 20),
        cost_estimate=pl.CostEstimate(flops=8 * t * size, bytes_accessed=4 * size, transcendentals=0),
    )(head, *[v for p in pairs for v in p])


def solution(mesh):
    n = mesh.shape['tp']
    half = n // 2

    def hop(v, d):
        return lax.ppermute(v, 'tp', [(2 * k + c, 2 * ((k + d) % half) + c) for k in range(half) for c in range(2)])

    def body(x, dy, w1, w2):
        xg, dyg, z, dz, own, plus, minus, opp, head = _forward(x, dy, w1, w2, n)
        parts = [hop(plus, 1), hop(minus, half - 1), hop(opp, 2)]
        dw2, dw1 = _wgrads(head, [(z, dyg), (xg, dz)], 256)
        dx = own
        for p in parts:
            dx = dx + p.astype(F32)
        return dx.astype(BF16), dw1, dw2

    return jax.shard_map(
        body, mesh=mesh,
        in_specs=(P(('dp', 'tp'), None), P(('dp', 'tp'), None), P(None, 'tp'), P('tp', None)),
        out_specs=(P(('dp', 'tp'), None), P('dp', 'tp'), P(('dp', 'tp'), None)),
        check_vma=False)
```
